512 devices in a mesh: gx: 16 (over y_hi, x), gy: 32 (over y_lo, z, core).
Axes of the slice: x: 4, y: 8 (y_hi: 4, y_lo: 2; y = y_hi * 2 + y_lo), z: 8, core: 2. Of those that a mesh axis runs over, the one named last changes fastest.
Arguments:
- density: float32 [16, 1024, 4096], P(None, 'gx', 'gy'), may hold values from 0.1 to 1
- cotangent: float32 [16, 1024, 4096], P(None, 'gx', 'gy'), may hold values from -6 to 6
Outputs:
- printed: float32 [16, 1024, 4096], P(None, 'gx', 'gy')
- gradient: float32 [16, 1024, 4096], P(None, 'gx', 'gy')
The draws below stay inside these ranges and needn't reach their ends.
All inputs are finite; a program needn't handle non-finite values.
Results may differ from the reference program's by a relative error of at most 0.0003.
Values sent between devices are 32-bit elements; how exact they have to be, the bound alone decides.
A program may use at most 64 MiB of HBM per device.

```python
import math
import jax
import jax.numpy as jnp
from jax import lax

NZ = 16
NX = 1024
NY = 4096


def draw_density(key, part):
    key_pillar = jax.random.fold_in(key, 11)
    key_level = jax.random.fold_in(key, 23)
    picks = jax.random.randint(key_pillar, (NX, NY), 0, 400)
    pillar = picks == 0
    spread = jax.random.uniform(key_level, (NZ, NX, NY), jnp.float32)
    upper = 0.85 + 0.15 * spread
    base = 0.1 + 0.1 * spread
    summit = 0.95 + 0.05 * spread
    ground = jnp.where(pillar[None], summit, base)
    layers = jnp.arange(NZ, dtype=jnp.int32)[:, None, None]
    return jnp.where(layers == 0, ground, upper).astype(jnp.float32)


def steps_of(key, shape, cuts, low, high):
    gain = 1.0
    for position, blocks in cuts:
        draws = jax.random.uniform(jax.random.fold_in(jax.random.fold_in(key, 6), position), (blocks,), jnp.float32, low / len(cuts), high / len(cuts))
        gain = gain * jnp.repeat(jnp.exp(draws), shape[position] // blocks).reshape((-1,) + (1,) * (len(shape) - 1 - position))
    return gain


def centred(own_key, dims, deviation, most, pieces=(), held_as=jnp.bfloat16):
    entries = jax.random.normal(own_key, dims, jnp.float32) * deviation
    if len(pieces) > 0:
        entries = steps_of(own_key, dims, pieces, -0.22, 0.18) * entries
    return jnp.clip(entries, min=-most, max=most).astype(held_as)


def setup_inputs(seed: int = 0) -> dict:
    seeds = jax.random.split(jax.random.key(seed), 3)
    density = draw_density(jax.random.fold_in(seeds[2], 71), 0)
    cotangent = centred(seeds[1], (NZ, NX, NY), 1.0, 6.0, ((1, 16), (2, 32)), jnp.float32)
    return dict(density=density, cotangent=cotangent)


power_p = 20.0
root_q = 20.0 + math.log(5.0) / math.log(0.1)
smooth_eps = 0.0001

def cross_roll(plane):
    return plane + jnp.roll(plane, 1, 0) + jnp.roll(plane, -1, 0) + jnp.roll(plane, 1, 1) + jnp.roll(plane, -1, 1)

def reference(density, cotangent):
    layers = jnp.arange(density.shape[0], dtype=jnp.int32)

    def forward(prev, inputs):
        plane, zval = inputs
        total = cross_roll(prev ** power_p)
        level = jnp.where(zval == 0, jnp.float32(1.0), total ** (1.0 / root_q))
        diff = plane - level
        printed_layer = 0.5 * (plane + level - jnp.sqrt(diff * diff + smooth_eps) + math.sqrt(smooth_eps))
        return (printed_layer, printed_layer)
    start = jnp.ones(density.shape[1:], jnp.float32)
    last, printed = lax.scan(forward, start, (density, layers))
    below = jnp.concatenate([start[None], printed[:-1]], 0)

    def backward(carried, inputs):
        grad_in, plane, here, under, zval = inputs
        adjoint = grad_in + power_p / root_q * here ** (power_p - 1.0) * cross_roll(carried)
        total = cross_roll(under ** power_p)
        level = jnp.where(zval == 0, jnp.float32(1.0), total ** (1.0 / root_q))
        diff = plane - level
        root = jnp.sqrt(diff * diff + smooth_eps)
        grad_layer = adjoint * 0.5 * (1.0 - diff / root)
        carried_next = adjoint * 0.5 * (1.0 + diff / root) * level / total
        return (carried_next, grad_layer)
    zero_state = jnp.zeros(density.shape[1:], jnp.float32)
    final, gradient = lax.scan(backward, zero_state, (cotangent, density, printed, below, layers), reverse=True)
    return (printed, gradient)
```

```python
import math

import jax
import jax.numpy as jnp
from jax import lax
from jax.experimental import pallas as pl
from jax.experimental.pallas import tpu as pltpu
from jax.sharding import PartitionSpec as P

power_p = 20.0
root_q = 20.0 + math.log(5.0) / math.log(0.1)
smooth_eps = 0.0001

NZ = 16
ROWS = 64
LANES = 128
WIDE = 32
NEAR = 16
F32 = jnp.float32
MESH = pl.DeviceIdType.MESH

REACH = [2 * (NZ - 1) - z for z in range(NZ)]


def up8(n):
    return (n + 7) // 8 * 8


def place(counts):
    out, vec, first, last, prev = [], 0, None, 0, 0
    for n in counts:
        if first is None:
            off, first = 0, n
        else:
            off = last + max(prev, n)
            if off > LANES - first or off + n > LANES:
                vec, off, first = vec + 1, 0, n
        out.append((vec, off))
        last, prev = off, n
    return out, vec + 1


def stream(order, width):
    starts, chunks, at, sent = {}, [], 0, 0
    for z in order:
        starts[z] = at
        at += width(z)
        end = up8(at)
        chunks.append((sent, end - sent))
        sent = end
    return starts, chunks, sent


class Plan:
    def __init__(self, order, width, merges):
        self.order, self.width = order, width
        self.starts, chunks, self.rows = stream(order, width)
        self.row_chunks, self.row_need, at = [], {}, 0
        for count in merges:
            part = chunks[at : at + count]
            for z in order[at : at + count]:
                self.row_need[z] = len(self.row_chunks)
            self.row_chunks.append((part[0][0], sum(n for _, n in part)))
            at += count
        places, self.col_vecs = place([width(z) for z in order])
        self.cols = {z: p for z, p in zip(order, places)}
        self.corners, base = {}, 0
        firsts = []
        for bands in ((0,), (1,), (2, 3)):
            items = [
                (z, b, width(z) - 8 * b - 1)
                for b in bands
                for z in order
                if width(z) - 8 * b - 1 > 0
            ]
            if not items:
                continue
            places, vecs = place([n for _, _, n in items])
            for (z, b, n), (vec, off) in zip(items, places):
                self.corners[(z, b)] = (base + vec, off, n)
            for vec in range(vecs):
                firsts.append(min(order.index(z) for (z, b, n), p in zip(items, places) if p[0] == vec))
            base += vecs
        rank = sorted(range(base), key=lambda v: firsts[v])
        where = {v: i for i, v in enumerate(rank)}
        self.corners = {k: (where[v], o, n) for k, (v, o, n) in self.corners.items()}
        self.corner_vecs = base
        self.corner_chunks, self.corner_first = [], []
        for i, v in enumerate(rank):
            if self.corner_first and firsts[v] == self.corner_first[-1]:
                at, n = self.corner_chunks[-1]
                self.corner_chunks[-1] = (at, n + 8)
            else:
                self.corner_chunks.append((8 * i, 8))
                self.corner_first.append(firsts[v])

    def corner_need(self, z):
        need = -1
        for (layer, _), (vec, _, _) in self.corners.items():
            if layer == z:
                for i, (at, n) in enumerate(self.corner_chunks):
                    if at <= 8 * vec < at + n:
                        need = max(need, i)
        return need


DENS = Plan(list(range(NZ)), lambda z: REACH[z], [1] * NZ)
COTS = Plan(list(range(NZ - 1, 0, -1)), lambda z: z, [1, 1, 2, 4, 7])
PLANS = (DENS, COTS)


def messages(plan):
    out, seen = [], set()
    for i, z in enumerate(plan.order):
        wanted = [("row", plan.row_need[z])]
        if plan.corner_need(z) >= 0:
            wanted += [("corner", c) for c in range(plan.corner_need(z) + 1)]
        wanted += [("col", plan.cols[z][0])]
        for m in wanted:
            if m not in seen:
                seen.add(m)
                out.append(m)
    return out


COPIES = [messages(plan) for plan in PLANS]
SLOTS = [[(kind, c) for kind, c in copies for _ in range(4 if kind == "corner" else 2)] for copies in COPIES]
N_SEMS = sum(len(s) for s in SLOTS)


def lane_ids(shape):
    return lax.broadcasted_iota(jnp.int32, shape, len(shape) - 1)


def rotate(x, shift, axis=None):
    shift = shift % LANES
    if shift == 0:
        return x
    return pltpu.roll(x, shift, x.ndim - 1 if axis is None else axis)


def cross(ref, lo, hi):
    here = ref[:, lo:hi, :]
    lane = lane_ids(here.shape)
    east = rotate(here, 1)
    west = rotate(here, LANES - 1)
    swap = lambda v: jnp.concatenate([v[1:], v[:1]], axis=0)
    return (
        here
        + ref[:, lo - 1 : hi - 1, :]
        + ref[:, lo + 1 : hi + 1, :]
        + jnp.where(lane == 0, swap(east), east)
        + jnp.where(lane == LANES - 1, swap(west), west)
    )


def spans(margin, halo):
    out = []
    if halo:
        out.append((margin - halo, margin))
    out += [(margin, margin + ROWS // 2), (margin + ROWS // 2, margin + ROWS)]
    if halo:
        out.append((margin + ROWS, margin + ROWS + halo))
    return out


def kernel(
    dens_hbm,
    cots_hbm,
    printed_ref,
    grad_ref,
    dens,
    cots,
    t_even,
    t_odd,
    k_even,
    k_odd,
    coef,
    weight,
    shrink,
    row_out_d,
    row_in_d,
    col_out_d,
    col_in_d,
    cor_out_d,
    cor_in_d,
    row_out_c,
    row_in_c,
    col_out_c,
    col_in_c,
    cor_out_c,
    cor_in_c,
    load_sem,
    send_sem,
    recv_sem,
):
    gx, gy = lax.axis_index("gx"), lax.axis_index("gy")
    nx, ny = lax.axis_size("gx"), lax.axis_size("gy")
    up, down = lax.rem(gx + nx - 1, nx), lax.rem(gx + 1, nx)
    left, right = lax.rem(gy + ny - 1, ny), lax.rem(gy + 1, ny)

    load_d = pltpu.make_async_copy(dens_hbm, dens.at[:, 0, WIDE : WIDE + ROWS], load_sem.at[0])
    load_c = pltpu.make_async_copy(cots_hbm, cots.at[:, 0, NEAR : NEAR + ROWS], load_sem.at[1])
    load_d.start()
    load_c.start()

    barrier = pltpu.get_barrier_semaphore()
    for x, y in (
        (up, gy), (down, gy), (gx, left), (gx, right),
        (up, left), (up, right), (down, left), (down, right),
    ):
        pl.semaphore_signal(barrier, inc=1, device_id={"gx": x, "gy": y}, device_id_type=MESH)

    bufs = (
        (dens, WIDE, (row_out_d, col_out_d, cor_out_d), (row_in_d, col_in_d, cor_in_d)),
        (cots, NEAR, (row_out_c, col_out_c, cor_out_c), (row_in_c, col_in_c, cor_in_c)),
    )

    def pack(which):
        plan = PLANS[which]
        src, margin, (row, col, cor), _ = bufs[which]
        for z in plan.order:
            w, at = plan.width(z), plan.starts[z]
            row[0, at : at + w, :] = src[z, 0, margin : margin + w, :]
            row[1, at : at + w, :] = src[z, 0, margin + ROWS - w : margin + ROWS, :]
        for vec in range(plan.col_vecs):
            lane = lane_ids((ROWS, LANES))
            low = high = None
            for z in plan.order:
                v, off = plan.cols[z]
                if v != vec:
                    continue
                w = plan.width(z)
                turned = rotate(src[z, 0, margin : margin + ROWS, :], off)
                if low is None:
                    low = high = turned
                else:
                    low = jnp.where(lane >= off, turned, low)
                    high = jnp.where((lane >= off - w) & (lane < off), turned, high)
            col[0, vec * ROWS : (vec + 1) * ROWS, :] = low
            col[1, vec * ROWS : (vec + 1) * ROWS, :] = high
        lane = lane_ids((8, LANES))
        for vec in range(plan.corner_vecs):
            for side in range(2):
                low = high = None
                for (z, b), (v, off, n) in plan.corners.items():
                    if v != vec:
                        continue
                    lo = margin + 8 * b if side == 0 else margin + ROWS - 8 * (b + 1)
                    turned = rotate(src[z, 0, lo : lo + 8, :], off)
                    if low is None:
                        low = high = turned
                    else:
                        low = jnp.where(lane >= off, turned, low)
                        high = jnp.where((lane >= off - n) & (lane < off), turned, high)
                cor[2 * side, 8 * vec : 8 * vec + 8, :] = low
                cor[2 * side + 1, 8 * vec : 8 * vec + 8, :] = high

    copies = ({}, {})
    count = 0
    for which, plan in enumerate(PLANS):
        _, _, outs, ins = bufs[which]
        for kind, c in COPIES[which]:
            made = []
            if kind == "row":
                at, n = plan.row_chunks[c]
                targets = [(0, up, gy), (1, down, gy)]
                src, dst = outs[0], ins[0]
            elif kind == "col":
                at, n = c * ROWS, ROWS
                targets = [(0, gx, left), (1, gx, right)]
                src, dst = outs[1], ins[1]
            else:
                at, n = plan.corner_chunks[c]
                targets = [(0, up, left), (1, up, right), (2, down, left), (3, down, right)]
                src, dst = outs[2], ins[2]
            for i, x, y in targets:
                made.append(
                    pltpu.make_async_remote_copy(
                        src_ref=src.at[i, at : at + n],
                        dst_ref=dst.at[i, at : at + n],
                        send_sem=send_sem.at[count],
                        recv_sem=recv_sem.at[count],
                        device_id={"gx": x, "gy": y},
                        device_id_type=MESH,
                    )
                )
                count += 1
            copies[which][(kind, c)] = made

    load_d.wait()
    pack(0)
    load_c.wait()
    pack(1)
    pl.semaphore_wait(barrier, 8)
    for which in range(2):
        for m in COPIES[which]:
            for copy in copies[which][m]:
                copy.start()

    arrived = (set(), set())

    def receive(which, z):
        plan = PLANS[which]
        dst, margin, _, (row, col, cor) = bufs[which]
        wanted = [("row", c) for c in range(plan.row_need[z] + 1)]
        wanted += [("corner", c) for c in range(plan.corner_need(z) + 1)]
        wanted += [("col", c) for c in range(plan.cols[z][0] + 1)]
        for m in wanted:
            if m not in arrived[which]:
                arrived[which].add(m)
                for copy in copies[which][m]:
                    copy.wait_recv()
        w, at = plan.width(z), plan.starts[z]
        dst[z, 0, margin + ROWS : margin + ROWS + w, :] = row[0, at : at + w, :]
        dst[z, 0, margin - w : margin, :] = row[1, at : at + w, :]
        vec, off = plan.cols[z]
        lane = lane_ids((ROWS, LANES))
        part = slice(vec * ROWS, (vec + 1) * ROWS)
        both = jnp.where((lane >= off) & (lane < off + w), col[0, part, :], col[1, part, :])
        dst[z, 1, margin : margin + ROWS, :] = rotate(both, LANES - off)
        lane = lane_ids((8, LANES))
        for b in range(4):
            if (z, b) not in plan.corners:
                continue
            vec, off, n = plan.corners[(z, b)]
            part = slice(8 * vec, 8 * vec + 8)
            slot = (lane >= off) & (lane < off + n)
            low = jnp.where(slot, cor[0, part, :], cor[1, part, :])
            high = jnp.where(slot, cor[2, part, :], cor[3, part, :])
            lo = margin + ROWS + 8 * b
            dst[z, 1, lo : lo + 8, :] = rotate(low, LANES - off)
            lo = margin - 8 * (b + 1)
            dst[z, 1, lo : lo + 8, :] = rotate(high, LANES - off)

    towers = (t_even, t_odd)
    inner = WIDE - NEAR
    for z in range(NZ):
        receive(0, z)
        below, above = towers[(z + 1) % 2], towers[z % 2]
        for lo, hi in spans(WIDE, up8(REACH[z])):
            plane = dens[z, :, lo:hi, :]
            if z == 0:
                level = jnp.ones_like(plane)
            else:
                total = cross(below, lo + 8, hi + 8)
                logs = jnp.log(total)
                level = jnp.exp(logs * (1.0 / root_q))
            diff = plane - level
            square = diff * diff + smooth_eps
            inverse = lax.rsqrt(square)
            layer = 0.5 * (plane + level - square * inverse) + 0.5 * math.sqrt(smooth_eps)
            p2 = layer * layer
            p4 = p2 * p2
            p8 = p4 * p4
            p16 = p8 * p8
            p19 = p16 * (p2 * layer)
            if z < NZ - 1:
                above[:, lo + 8 : hi + 8, :] = p19 * layer
            near_lo, near_hi = max(lo, WIDE - up8(z)), min(hi, WIDE + ROWS + up8(z))
            if near_lo < near_hi:
                cut = lambda v: v[:, near_lo - lo : near_hi - lo, :]
                tilt = 0.5 * (cut(diff) * cut(inverse))
                coef[z, :, near_lo - inner : near_hi - inner, :] = (power_p / root_q) * cut(p19)
                if z > 0:
                    weight[z, :, near_lo - inner : near_hi - inner, :] = (0.5 + tilt) * jnp.exp(
                        cut(logs) * (1.0 / root_q - 1.0)
                    )
                if WIDE <= lo and hi <= WIDE + ROWS:
                    printed_ref[z, lo - WIDE : hi - WIDE, :] = layer[0]
                    shrink[z, lo - WIDE : hi - WIDE, :] = 0.5 - tilt[0]

    carried = (k_even, k_odd)
    for z in reversed(range(NZ)):
        if z > 0:
            receive(1, z)
        above, here = carried[(z + 1) % 2], carried[z % 2]
        for lo, hi in spans(NEAR, up8(z)):
            if z == 0:
                adjoint = cots[z, 0, lo:hi, :] + coef[z, 0, lo:hi, :] * cross(above, lo + 8, hi + 8)[0]
            elif z == NZ - 1:
                adjoint = cots[z, :, lo:hi, :]
            else:
                adjoint = cots[z, :, lo:hi, :] + coef[z, :, lo:hi, :] * cross(above, lo + 8, hi + 8)
            if z > 0:
                here[:, lo + 8 : hi + 8, :] = adjoint * weight[z, :, lo:hi, :]
            if NEAR <= lo and hi <= NEAR + ROWS:
                own = adjoint if z == 0 else adjoint[0]
                rows = slice(lo - NEAR, hi - NEAR)
                grad_ref[z, rows, :] = own * shrink[z, rows, :]

    for which in range(2):
        for m in COPIES[which]:
            for copy in copies[which][m]:
                copy.wait_send()


def shards(density, cotangent):
    def packed(plan):
        out = []
        for shape in ((2, plan.rows, LANES), (2, plan.col_vecs * ROWS, LANES), (4, 8 * plan.corner_vecs, LANES)):
            out += [pltpu.VMEM(shape, F32)] * 2
        return out

    wide, near = 2 * WIDE + ROWS, 2 * NEAR + ROWS
    shape = jax.ShapeDtypeStruct(density.shape, F32)
    return pl.pallas_call(
        kernel,
        out_shape=(shape, shape),
        in_specs=[pl.BlockSpec(memory_space=pl.ANY)] * 2,
        out_specs=(pl.BlockSpec(memory_space=pltpu.VMEM),) * 2,
        scratch_shapes=[
            pltpu.VMEM((NZ, 2, wide, LANES), F32),
            pltpu.VMEM((NZ, 2, near, LANES), F32),
            pltpu.VMEM((2, wide + 16, LANES), F32),
            pltpu.VMEM((2, wide + 16, LANES), F32),
            pltpu.VMEM((2, near + 16, LANES), F32),
            pltpu.VMEM((2, near + 16, LANES), F32),
            pltpu.VMEM((NZ, 2, near, LANES), F32),
            pltpu.VMEM((NZ, 2, near, LANES), F32),
            pltpu.VMEM((NZ, ROWS, LANES), F32),
            *packed(DENS),
            *packed(COTS),
            pltpu.SemaphoreType.DMA((2,)),
            pltpu.SemaphoreType.DMA((N_SEMS,)),
            pltpu.SemaphoreType.DMA((N_SEMS,)),
        ],
        compiler_params=pltpu.CompilerParams(collective_id=0, has_side_effects=True),
    )(density, cotangent)


def solution(mesh):
    placed = (P(None, "gx", "gy"), P(None, "gx", "gy"))
    return jax.shard_map(
        shards,
        mesh=mesh,
        in_specs=placed,
        out_specs=placed,
        check_vma=False,
    )
```

```python
import math

import jax
import jax.numpy as jnp
from jax import lax
from jax.experimental import pallas as pl
from jax.experimental.pallas import tpu as pltpu
from jax.sharding import PartitionSpec as P

power_p = 20.0
root_q = 20.0 + math.log(5.0) / math.log(0.1)
smooth_eps = 0.0001

NZ = 16
ROWS = 64
LANES = 128
WIDE = 32
NEAR = 16
F32 = jnp.float32
MESH = pl.DeviceIdType.MESH

REACH = [2 * (NZ - 1) - z for z in range(NZ)]


def up8(n):
    return (n + 7) // 8 * 8


def place(counts):
    out, vec, first, last, prev = [], 0, None, 0, 0
    for n in counts:
        if first is None:
            off, first = 0, n
        else:
            off = last + max(prev, n)
            if off > LANES - first or off + n > LANES:
                vec, off, first = vec + 1, 0, n
        out.append((vec, off))
        last, prev = off, n
    return out, vec + 1


def stream(order, width):
    starts, chunks, at, sent = {}, [], 0, 0
    for z in order:
        starts[z] = at
        at += width(z)
        end = up8(at)
        chunks.append((sent, end - sent))
        sent = end
    return starts, chunks, sent


class Plan:
    def __init__(self, order, width, merges):
        self.order, self.width = order, width
        self.starts, chunks, self.rows = stream(order, width)
        self.row_chunks, self.row_need, at = [], {}, 0
        for count in merges:
            part = chunks[at : at + count]
            for z in order[at : at + count]:
                self.row_need[z] = len(self.row_chunks)
            self.row_chunks.append((part[0][0], sum(n for _, n in part)))
            at += count
        places, self.col_vecs = place([width(z) for z in order])
        self.cols = {z: p for z, p in zip(order, places)}
        self.corners, base = {}, 0
        firsts = []
        for bands in ((0,), (1,), (2, 3)):
            items = [
                (z, b, width(z) - 8 * b - 1)
                for b in bands
                for z in order
                if width(z) - 8 * b - 1 > 0
            ]
            if not items:
                continue
            places, vecs = place([n for _, _, n in items])
            for (z, b, n), (vec, off) in zip(items, places):
                self.corners[(z, b)] = (base + vec, off, n)
            for vec in range(vecs):
                firsts.append(min(order.index(z) for (z, b, n), p in zip(items, places) if p[0] == vec))
            base += vecs
        rank = sorted(range(base), key=lambda v: firsts[v])
        where = {v: i for i, v in enumerate(rank)}
        self.corners = {k: (where[v], o, n) for k, (v, o, n) in self.corners.items()}
        self.corner_vecs = base
        self.corner_chunks, self.corner_first = [], []
        for i, v in enumerate(rank):
            if self.corner_first and firsts[v] == self.corner_first[-1]:
                at, n = self.corner_chunks[-1]
                self.corner_chunks[-1] = (at, n + 8)
            else:
                self.corner_chunks.append((8 * i, 8))
                self.corner_first.append(firsts[v])

    def corner_need(self, z):
        need = -1
        for (layer, _), (vec, _, _) in self.corners.items():
            if layer == z:
                for i, (at, n) in enumerate(self.corner_chunks):
                    if at <= 8 * vec < at + n:
                        need = max(need, i)
        return need


DENS = Plan(list(range(NZ)), lambda z: REACH[z], [1] * 8 + [2] * 4)
COTS = Plan(list(range(NZ - 1, 0, -1)), lambda z: z, [1, 1, 2, 4, 7])
PLANS = (DENS, COTS)

RELAYED = [(0, 8), (0, 9), (0, 10), (0, 11), (1, 0), (1, 1), (1, 2), (1, 3), (1, 4)]
PASS_ON = {1: [4], 2: [5], 3: [6], 4: [7], 5: [8]}


def messages(plan):
    out, seen = [], set()
    for i, z in enumerate(plan.order):
        wanted = [("corner", c) for c in range(len(plan.corner_chunks))]
        wanted += [("row", plan.row_need[z])]
        wanted += [("col", plan.cols[z][0])]
        for m in wanted:
            if m not in seen:
                seen.add(m)
                out.append(m)
    return out


COPIES = [messages(plan) for plan in PLANS]
SLOTS = [[(kind, c) for kind, c in copies for _ in range(4 if kind == "corner" else 2)] for copies in COPIES]
N_SEMS = sum(len(s) for s in SLOTS)


OPPOSITE = (1, 0, 3, 2, 7, 6, 5, 4, 9, 8, 10)
URGENT = (7, 5, 3)
TOKEN_ORDER = (3, 1, 10, 7, 0, 8, 9, 5, 2, 6, 4)


def rank(gx, gy):
    x, y = lax.rem(gx, 4), 2 * lax.div(gx, 4) + lax.div(gy, 16)
    z, core = lax.rem(lax.div(gy, 2), 8), lax.rem(gy, 2)
    far = lax.div(y, 4)
    hops = y * (1 - 2 * far) + 8 * far
    first = 1 - lax.div(gx * 32 + gy + 511, 512)
    return 13 * z + 8 * hops + 9 * x + 4 * (1 - core) + 60 * first


def lane_ids(shape):
    return lax.broadcasted_iota(jnp.int32, shape, len(shape) - 1)


def rotate(x, shift, axis=None):
    shift = shift % LANES
    if shift == 0:
        return x
    return pltpu.roll(x, shift, x.ndim - 1 if axis is None else axis)


def cross(ref, lo, hi):
    here = ref[:, lo:hi, :]
    lane = lane_ids(here.shape)
    east = rotate(here, 1)
    west = rotate(here, LANES - 1)
    swap = lambda v: jnp.concatenate([v[1:], v[:1]], axis=0)
    return (
        here
        + ref[:, lo - 1 : hi - 1, :]
        + ref[:, lo + 1 : hi + 1, :]
        + jnp.where(lane == 0, swap(east), east)
        + jnp.where(lane == LANES - 1, swap(west), west)
    )


def spans(margin, halo):
    out = []
    if halo:
        out.append((margin - halo, margin))
    out += [(margin, margin + ROWS // 2), (margin + ROWS // 2, margin + ROWS)]
    if halo:
        out.append((margin + ROWS, margin + ROWS + halo))
    return out


def kernel(
    dens_hbm,
    cots_hbm,
    printed_ref,
    grad_ref,
    dens,
    cots,
    t_even,
    t_odd,
    k_even,
    k_odd,
    coef,
    weight,
    shrink,
    relay_d,
    relay_c,
    row_out_d,
    row_in_d,
    col_out_d,
    col_in_d,
    cor_out_d,
    cor_in_d,
    row_out_c,
    row_in_c,
    col_out_c,
    col_in_c,
    cor_out_c,
    cor_in_c,
    load_sem,
    send_sem,
    recv_sem,
    token_sem,
    relay_send,
    relay_recv,
):
    gx, gy = lax.axis_index("gx"), lax.axis_index("gy")
    nx, ny = lax.axis_size("gx"), lax.axis_size("gy")
    up, down = lax.rem(gx + nx - 1, nx), lax.rem(gx + 1, nx)
    left, right = lax.rem(gy + ny - 1, ny), lax.rem(gy + 1, ny)

    load_d = pltpu.make_async_copy(dens_hbm, dens.at[:, 0, WIDE : WIDE + ROWS], load_sem.at[0])
    load_c = pltpu.make_async_copy(cots_hbm, cots.at[:, 0, NEAR : NEAR + ROWS], load_sem.at[1])
    load_d.start()
    load_c.start()

    around = (
        (up, gy), (down, gy), (gx, left), (gx, right),
        (up, left), (up, right), (down, left), (down, right),
        (lax.rem(gx + 4, nx), gy), (lax.rem(gx + nx - 4, nx), gy), (gx + 3 - 2 * lax.rem(gx, 4), gy),
    )
    mine = rank(gx, gy)
    low_end, high_end = lax.rem(gx, 4) == 0, lax.rem(gx, 4) == 3
    at_end = jnp.logical_or(low_end, high_end)
    ends = (low_end, high_end, None, None, low_end, low_end, high_end, high_end)
    later, ready, earlier, greets = [], [], [], []
    for d, (x, y) in enumerate(around):
        lag = rank(x, y) - mine
        slack = 20 if d < 4 else 0 if d < 8 else 30
        if d < 8 and ends[d] is not None:
            slack = slack + (30 - slack) * ends[d].astype(jnp.int32)
        later.append(lag > slack)
        ready.append(lag <= slack)
        mutual = jnp.logical_and(lag <= slack, lag >= -slack)
        earlier.append(lag < -slack)
        greets.append(jnp.logical_or(lag > slack, mutual))
    for d in range(8, 11):
        for flags in (later, ready, earlier, greets):
            flags[d] = jnp.logical_and(at_end, flags[d])
    barrier = pltpu.get_barrier_semaphore()
    for d, (x, y) in enumerate(around):
        pl.when(greets[d])(
            lambda x=x, y=y: pl.semaphore_signal(
                barrier, inc=1, device_id={"gx": x, "gy": y}, device_id_type=MESH
            )
        )
    pl.semaphore_wait(barrier, sum(v.astype(jnp.int32) for v in ready))
    for d, (x, y) in enumerate(around):
        pl.when(earlier[d])(
            lambda d=d, x=x, y=y: pl.semaphore_signal(
                token_sem.at[OPPOSITE[d]], inc=1, device_id={"gx": x, "gy": y}, device_id_type=MESH
            )
        )

    bufs = (
        (dens, WIDE, (row_out_d, col_out_d, cor_out_d), (row_in_d, col_in_d, cor_in_d)),
        (cots, NEAR, (row_out_c, col_out_c, cor_out_c), (row_in_c, col_in_c, cor_in_c)),
    )

    def pack(which):
        plan = PLANS[which]
        src, margin, (row, col, cor), _ = bufs[which]
        for z in plan.order:
            w, at = plan.width(z), plan.starts[z]
            row[0, at : at + w, :] = src[z, 0, margin : margin + w, :]
            row[1, at : at + w, :] = src[z, 0, margin + ROWS - w : margin + ROWS, :]
        for vec in range(plan.col_vecs):
            lane = lane_ids((ROWS, LANES))
            low = high = None
            for z in plan.order:
                v, off = plan.cols[z]
                if v != vec:
                    continue
                w = plan.width(z)
                turned = rotate(src[z, 0, margin : margin + ROWS, :], off)
                if low is None:
                    low = high = turned
                else:
                    low = jnp.where(lane >= off, turned, low)
                    high = jnp.where((lane >= off - w) & (lane < off), turned, high)
            col[0, vec * ROWS : (vec + 1) * ROWS, :] = low
            col[1, vec * ROWS : (vec + 1) * ROWS, :] = high
        lane = lane_ids((8, LANES))
        for vec in range(plan.corner_vecs):
            for side in range(2):
                low = high = None
                for (z, b), (v, off, n) in plan.corners.items():
                    if v != vec:
                        continue
                    lo = margin + 8 * b if side == 0 else margin + ROWS - 8 * (b + 1)
                    turned = rotate(src[z, 0, lo : lo + 8, :], off)
                    if low is None:
                        low = high = turned
                    else:
                        low = jnp.where(lane >= off, turned, low)
                        high = jnp.where((lane >= off - n) & (lane < off), turned, high)
                cor[2 * side, 8 * vec : 8 * vec + 8, :] = low
                cor[2 * side + 1, 8 * vec : 8 * vec + 8, :] = high

    copies, order = ({}, {}), ([], [])
    relays, hops, vias = (relay_d, relay_c), [[] for _ in RELAYED], {}
    count = 0
    for which, plan in enumerate(PLANS):
        _, _, outs, ins = bufs[which]
        for kind, c in COPIES[which]:
            made = []
            if kind == "row":
                at, n = plan.row_chunks[c]
                targets = [(0, 0), (1, 1)]
                src, dst = outs[0], ins[0]
            elif kind == "col":
                at, n = c * ROWS, ROWS
                targets = [(0, 2), (1, 3)]
                src, dst = outs[1], ins[1]
            else:
                at, n = plan.corner_chunks[c]
                targets = [(0, 4), (1, 5), (2, 6), (3, 7)]
                src, dst = outs[2], ins[2]
            for i, d in targets:
                x, y = around[d]
                copy = (
                    pltpu.make_async_remote_copy(
                        src_ref=src.at[i, at : at + n],
                        dst_ref=dst.at[i, at : at + n],
                        send_sem=send_sem.at[8 * which + d],
                        recv_sem=recv_sem.at[count],
                        device_id={"gx": x, "gy": y},
                        device_id_type=MESH,
                    )
                )
                made.append(copy)
                if (which, c) in RELAYED and kind == "row":
                    k = RELAYED.index((which, c))
                    end, beyond = ((low_end, 9), (high_end, 8))[i]
                    x, y = around[10]
                    via = pltpu.make_async_remote_copy(
                        src_ref=src.at[i, at : at + n],
                        dst_ref=relays[which].at[at : at + n],
                        send_sem=send_sem.at[8 * which + d],
                        recv_sem=relay_recv.at[k],
                        device_id={"gx": x, "gy": y},
                        device_id_type=MESH,
                    )
                    x, y = around[beyond]
                    onward = pltpu.make_async_remote_copy(
                        src_ref=relays[which].at[at : at + n],
                        dst_ref=dst.at[i, at : at + n],
                        send_sem=relay_send.at[which],
                        recv_sem=recv_sem.at[count],
                        device_id={"gx": x, "gy": y},
                        device_id_type=MESH,
                    )
                    order[which].append((d, copy, jnp.logical_not(end)))
                    order[which].append((10, via, end))
                    hops[k].append(onward)
                    vias[k] = via
                else:
                    order[which].append((d, copy, None))
                count += 1
            copies[which][(kind, c)] = made

    def sent(src, dst, sem):
        pltpu.make_async_remote_copy(
            src_ref=src,
            dst_ref=dst,
            send_sem=sem,
            recv_sem=recv_sem.at[0],
            device_id={"gx": up, "gy": gy},
            device_id_type=MESH,
        ).wait_send()

    load_d.wait()
    pack(0)

    def send(which, d, gate):
        for e, copy, on in order[which]:
            if d is not None and e != d:
                continue
            conds = [v for v in (gate[e] if gate else None, on) if v is not None]
            if not conds:
                copy.start()
            else:
                pl.when(conds[0] if len(conds) == 1 else jnp.logical_and(*conds))(copy.start)

    feeds = lax.rem(gy, 16) == 15
    usual = jnp.logical_not(feeds)
    first = [v if d in URGENT else jnp.logical_and(v, usual) for d, v in enumerate(ready)]
    after = [jnp.logical_and(v, feeds) for v in ready]
    send(0, None, first)
    load_c.wait()
    pack(1)

    def gone():
        for d in URGENT[:2]:
            sent(cor_out_d.at[d - 4], cor_in_d.at[d - 4], send_sem.at[d])

    pl.when(feeds)(gone)
    for d in range(11):
        if d not in URGENT:
            send(0, d, after)
    send(1, None, ready)

    def answer(d):
        pl.semaphore_wait(token_sem.at[d], 1)
        send(0, d, None)
        send(1, d, None)

    for d in TOKEN_ORDER:
        pl.when(later[d])(lambda d=d: answer(d))

    def pass_on(k):
        vias[k].wait_recv()
        pl.when(high_end)(hops[k][0].start)
        pl.when(low_end)(hops[k][1].start)

    arrived = (set(), set())

    def receive(which, z):
        plan = PLANS[which]
        dst, margin, _, (row, col, cor) = bufs[which]
        wanted = [("row", c) for c in range(plan.row_need[z] + 1)]
        wanted += [("corner", c) for c in range(plan.corner_need(z) + 1)]
        wanted += [("col", c) for c in range(plan.cols[z][0] + 1)]
        for m in wanted:
            if m not in arrived[which]:
                arrived[which].add(m)
                for copy in copies[which][m]:
                    copy.wait_recv()
        w, at = plan.width(z), plan.starts[z]
        dst[z, 0, margin + ROWS : margin + ROWS + w, :] = row[0, at : at + w, :]
        dst[z, 0, margin - w : margin, :] = row[1, at : at + w, :]
        vec, off = plan.cols[z]
        lane = lane_ids((ROWS, LANES))
        part = slice(vec * ROWS, (vec + 1) * ROWS)
        both = jnp.where((lane >= off) & (lane < off + w), col[0, part, :], col[1, part, :])
        dst[z, 1, margin : margin + ROWS, :] = rotate(both, LANES - off)
        lane = lane_ids((8, LANES))
        for b in range(4):
            if (z, b) not in plan.corners:
                continue
            vec, off, n = plan.corners[(z, b)]
            part = slice(8 * vec, 8 * vec + 8)
            slot = (lane >= off) & (lane < off + n)
            low = jnp.where(slot, cor[0, part, :], cor[1, part, :])
            high = jnp.where(slot, cor[2, part, :], cor[3, part, :])
            lo = margin + ROWS + 8 * b
            dst[z, 1, lo : lo + 8, :] = rotate(low, LANES - off)
            lo = margin - 8 * (b + 1)
            dst[z, 1, lo : lo + 8, :] = rotate(high, LANES - off)

    towers = (t_even, t_odd)
    inner = WIDE - NEAR
    waits = jnp.logical_and(at_end, later[2])
    busy = jnp.logical_and(at_end, jnp.logical_not(later[2]))
    for k, (which, _) in enumerate(RELAYED):
        pl.when(at_end if which == 0 else waits)(lambda k=k: pass_on(k))
    for z in range(NZ):
        for k in PASS_ON.get(z, []):
            pl.when(busy)(lambda k=k: pass_on(k))
        receive(0, z)
        below, above = towers[(z + 1) % 2], towers[z % 2]
        for lo, hi in spans(WIDE, up8(REACH[z])):
            plane = dens[z, :, lo:hi, :]
            if z == 0:
                level = jnp.ones_like(plane)
            else:
                total = cross(below, lo + 8, hi + 8)
                logs = jnp.log(total)
                level = jnp.exp(logs * (1.0 / root_q))
            diff = plane - level
            square = diff * diff + smooth_eps
            inverse = lax.rsqrt(square)
            layer = 0.5 * (plane + level - square * inverse) + 0.5 * math.sqrt(smooth_eps)
            p2 = layer * layer
            p4 = p2 * p2
            p8 = p4 * p4
            p16 = p8 * p8
            p19 = p16 * (p2 * layer)
            if z < NZ - 1:
                above[:, lo + 8 : hi + 8, :] = p19 * layer
            near_lo, near_hi = max(lo, WIDE - up8(z)), min(hi, WIDE + ROWS + up8(z))
            if near_lo < near_hi:
                cut = lambda v: v[:, near_lo - lo : near_hi - lo, :]
                tilt = 0.5 * (cut(diff) * cut(inverse))
                coef[z, :, near_lo - inner : near_hi - inner, :] = (power_p / root_q) * cut(p19)
                if z > 0:
                    weight[z, :, near_lo - inner : near_hi - inner, :] = (0.5 + tilt) * jnp.exp(
                        cut(logs) * (1.0 / root_q - 1.0)
                    )
                if WIDE <= lo and hi <= WIDE + ROWS:
                    printed_ref[z, lo - WIDE : hi - WIDE, :] = layer[0]
                    shrink[z, lo - WIDE : hi - WIDE, :] = 0.5 - tilt[0]

    carried = (k_even, k_odd)
    for z in reversed(range(NZ)):
        if z > 0:
            receive(1, z)
        above, here = carried[(z + 1) % 2], carried[z % 2]
        for lo, hi in spans(NEAR, up8(z)):
            if z == 0:
                adjoint = cots[z, 0, lo:hi, :] + coef[z, 0, lo:hi, :] * cross(above, lo + 8, hi + 8)[0]
            elif z == NZ - 1:
                adjoint = cots[z, :, lo:hi, :]
            else:
                adjoint = cots[z, :, lo:hi, :] + coef[z, :, lo:hi, :] * cross(above, lo + 8, hi + 8)
            if z > 0:
                here[:, lo + 8 : hi + 8, :] = adjoint * weight[z, :, lo:hi, :]
            if NEAR <= lo and hi <= NEAR + ROWS:
                own = adjoint if z == 0 else adjoint[0]
                rows = slice(lo - NEAR, hi - NEAR)
                grad_ref[z, rows, :] = own * shrink[z, rows, :]

    for which in range(2):
        _, _, outs, ins = bufs[which]
        for d in range(8):
            part, i = (0, d) if d < 2 else (1, d - 2) if d < 4 else (2, d - 4)
            args = (outs[part].at[i], ins[part].at[i], send_sem.at[8 * which + d])
            if which == 0 and d in URGENT[:2]:
                pl.when(usual)(lambda args=args: sent(*args))
            else:
                sent(*args)
        part = [PLANS[which].row_chunks[c] for w, c in RELAYED if w == which]
        lo, hi = part[0][0], part[-1][0] + part[-1][1]
        relay = relays[which].at[lo:hi]
        pl.when(at_end)(lambda relay=relay, which=which: sent(relay, relay, relay_send.at[which]))


def shards(density, cotangent):
    def packed(plan):
        out = []
        for shape in ((2, plan.rows, LANES), (2, plan.col_vecs * ROWS, LANES), (4, 8 * plan.corner_vecs, LANES)):
            out += [pltpu.VMEM(shape, F32)] * 2
        return out

    wide, near = 2 * WIDE + ROWS, 2 * NEAR + ROWS
    shape = pltpu.VMEM(density.shape, F32)
    results = pl.pallas_call(
        kernel,
        out_shape=(shape, shape),
        in_specs=[pl.BlockSpec(memory_space=pl.ANY)] * 2,
        out_specs=(pl.BlockSpec(memory_space=pltpu.VMEM),) * 2,
        scratch_shapes=[
            pltpu.VMEM((NZ, 2, wide, LANES), F32),
            pltpu.VMEM((NZ, 2, near, LANES), F32),
            pltpu.VMEM((2, wide + 16, LANES), F32),
            pltpu.VMEM((2, wide + 16, LANES), F32),
            pltpu.VMEM((2, near + 16, LANES), F32),
            pltpu.VMEM((2, near + 16, LANES), F32),
            pltpu.VMEM((NZ, 2, near, LANES), F32),
            pltpu.VMEM((NZ, 2, near, LANES), F32),
            pltpu.VMEM((NZ, ROWS, LANES), F32),
            pltpu.VMEM((DENS.rows, LANES), F32),
            pltpu.VMEM((COTS.rows, LANES), F32),
            *packed(DENS),
            *packed(COTS),
            pltpu.SemaphoreType.DMA((2,)),
            pltpu.SemaphoreType.DMA((16,)),
            pltpu.SemaphoreType.DMA((N_SEMS,)),
            pltpu.SemaphoreType.REGULAR((11,)),
            pltpu.SemaphoreType.DMA((2,)),
            pltpu.SemaphoreType.DMA((len(RELAYED),)),
        ],
        compiler_params=pltpu.CompilerParams(collective_id=0, has_side_effects=True),
    )(density, cotangent)
    final = jax.ShapeDtypeStruct(density.shape, F32)
    return pl.pallas_call(
        store,
        out_shape=(final, final),
        in_specs=[pl.BlockSpec(memory_space=pltpu.VMEM)] * 2,
        out_specs=(pl.BlockSpec(memory_space=pl.ANY),) * 2,
        scratch_shapes=[pltpu.SemaphoreType.DMA((8,))],
    )(*(pltpu.with_memory_space_constraint(v, pltpu.VMEM) for v in results))


def store(printed_ref, grad_ref, printed_hbm, grad_hbm, sem):
    copies = []
    for i in range(8):
        src, dst = ((printed_ref, printed_hbm), (grad_ref, grad_hbm))[i % 2]
        part = slice(4 * (i // 2), 4 * (i // 2) + 4)
        copies.append(pltpu.make_async_copy(src.at[part], dst.at[part], sem.at[i]))
    for copy in copies:
        copy.start()
    for copy in copies:
        copy.wait()


def solution(mesh):
    placed = (P(None, "gx", "gy"), P(None, "gx", "gy"))
    return jax.shard_map(
        shards,
        mesh=mesh,
        in_specs=placed,
        out_specs=placed,
        check_vma=False,
    )
```

```python
import math

import jax
import jax.numpy as jnp
from jax import lax
from jax.experimental import pallas as pl
from jax.experimental.pallas import tpu as pltpu
from jax.sharding import PartitionSpec as P

power_p = 20.0
root_q = 20.0 + math.log(5.0) / math.log(0.1)
smooth_eps = 0.0001

NZ = 16
ROWS = 64
LANES = 128
WIDE = 32
NEAR = 16
F32 = jnp.float32
MESH = pl.DeviceIdType.MESH

REACH = [2 * (NZ - 1) - z for z in range(NZ)]


def up8(n):
    return (n + 7) // 8 * 8


def place(counts, tight):
    out, vec, first, last, prev = [], 0, None, 0, 0
    for n in counts:
        if first is None:
            off, first = 0, n
        else:
            off = last + (prev if tight else max(prev, n))
            if off + n > LANES or (off > LANES - first and not tight):
                vec, off, first = vec + 1, 0, n
        out.append((vec, off))
        last, prev = off, n
    return out, vec + 1


def stream(order, width):
    starts, chunks, at, sent = {}, [], 0, 0
    for z in order:
        starts[z] = at
        at += width(z)
        end = up8(at)
        chunks.append((sent, end - sent))
        sent = end
    return starts, chunks, sent


class Plan:
    def __init__(self, order, width, merges, groups, tight):
        self.order, self.width = order, width
        self.starts, chunks, self.rows = stream(order, width)
        self.row_chunks, self.row_need, at = [], {}, 0
        for count in merges:
            part = chunks[at : at + count]
            for z in order[at : at + count]:
                self.row_need[z] = len(self.row_chunks)
            self.row_chunks.append((part[0][0], sum(n for _, n in part)))
            at += count
        places, self.col_vecs = place([width(z) for z in order], True)
        self.cols = {z: p for z, p in zip(order, places)}
        self.corners, base = {}, 0
        firsts = []
        self.tight = tight
        for bands in groups:
            items = [
                (z, b, width(z) - 8 * b - 1)
                for b in bands
                for z in order
                if width(z) - 8 * b - 1 > 0
            ]
            if not items:
                continue
            places, vecs = place([n for _, _, n in items], tight)
            for (z, b, n), (vec, off) in zip(items, places):
                self.corners[(z, b)] = (base + vec, off, n)
            for vec in range(vecs):
                firsts.append(min(order.index(z) for (z, b, n), p in zip(items, places) if p[0] == vec))
            base += vecs
        rank = sorted(range(base), key=lambda v: firsts[v])
        where = {v: i for i, v in enumerate(rank)}
        self.corners = {k: (where[v], o, n) for k, (v, o, n) in self.corners.items()}
        self.corner_vecs = base
        self.corner_chunks, self.corner_first = [], []
        for i, v in enumerate(rank):
            if self.corner_first and firsts[v] == self.corner_first[-1]:
                at, n = self.corner_chunks[-1]
                self.corner_chunks[-1] = (at, n + 8)
            else:
                self.corner_chunks.append((8 * i, 8))
                self.corner_first.append(firsts[v])

    def corner_need(self, z):
        need = -1
        for (layer, _), (vec, _, _) in self.corners.items():
            if layer == z:
                for i, (at, n) in enumerate(self.corner_chunks):
                    if at <= 8 * vec < at + n:
                        need = max(need, i)
        return need


DENS = Plan(list(range(NZ)), lambda z: REACH[z], [1] * 8 + [2] * 4, ((0,), (1,), (2, 3)), False)
COTS = Plan(list(range(NZ - 1, 0, -1)), lambda z: z, [1, 1, 2, 4, 7], ((0, 1),), True)
PLANS = (DENS, COTS)

RELAYED = [(0, 8), (0, 9), (0, 10), (0, 11), (1, 0), (1, 1), (1, 2), (1, 3), (1, 4)]
PASS_ON = {1: [4], 2: [5], 3: [6], 4: [7], 5: [8]}


def messages(plan):
    out, seen = [], set()
    for i, z in enumerate(plan.order):
        wanted = [("corner", c) for c in range(len(plan.corner_chunks))]
        wanted += [("row", plan.row_need[z])]
        wanted += [("col", plan.cols[z][0])]
        for m in wanted:
            if m not in seen:
                seen.add(m)
                out.append(m)
    return out


COPIES = [messages(plan) for plan in PLANS]
SLOTS = [[(kind, c) for kind, c in copies for _ in range(4 if kind == "corner" else 2)] for copies in COPIES]
N_SEMS = sum(len(s) for s in SLOTS)


OPPOSITE = (1, 0, 3, 2, 7, 6, 5, 4, 9, 8, 10)
URGENT = (7, 5, 3)
TOKEN_ORDER = (3, 1, 10, 7, 0, 8, 9, 5, 2, 6, 4)


def rank(gx, gy):
    x, y = lax.rem(gx, 4), 2 * lax.div(gx, 4) + lax.div(gy, 16)
    z, core = lax.rem(lax.div(gy, 2), 8), lax.rem(gy, 2)
    far = lax.div(y, 4)
    hops = y * (1 - 2 * far) + 8 * far
    first = 1 - lax.div(gx * 32 + gy + 511, 512)
    return 13 * z + 8 * hops + 9 * x + 4 * (1 - core) + 60 * first


def lane_ids(shape):
    return lax.broadcasted_iota(jnp.int32, shape, len(shape) - 1)


def rotate(x, shift, axis=None):
    shift = shift % LANES
    if shift == 0:
        return x
    return pltpu.roll(x, shift, x.ndim - 1 if axis is None else axis)


def cross(ref, lo, hi):
    here = ref[:, lo:hi, :]
    lane = lane_ids(here.shape)
    east = rotate(here, 1)
    west = rotate(here, LANES - 1)
    swap = lambda v: jnp.concatenate([v[1:], v[:1]], axis=0)
    return (
        here
        + ref[:, lo - 1 : hi - 1, :]
        + ref[:, lo + 1 : hi + 1, :]
        + jnp.where(lane == 0, swap(east), east)
        + jnp.where(lane == LANES - 1, swap(west), west)
    )


def spans(margin, halo):
    out = []
    if halo:
        out.append((margin - halo, margin))
    out += [(margin, margin + ROWS // 2), (margin + ROWS // 2, margin + ROWS)]
    if halo:
        out.append((margin + ROWS, margin + ROWS + halo))
    return out


def kernel(
    dens_hbm,
    cots_hbm,
    printed_ref,
    grad_ref,
    dens,
    cots,
    t_even,
    t_odd,
    k_even,
    k_odd,
    coef,
    weight,
    shrink,
    relay_d,
    relay_c,
    row_out_d,
    row_in_d,
    col_out_d,
    col_in_d,
    cor_out_d,
    cor_in_d,
    row_out_c,
    row_in_c,
    col_out_c,
    col_in_c,
    cor_out_c,
    cor_in_c,
    load_sem,
    send_sem,
    recv_sem,
    token_sem,
    relay_send,
    relay_recv,
):
    gx, gy = lax.axis_index("gx"), lax.axis_index("gy")
    nx, ny = lax.axis_size("gx"), lax.axis_size("gy")
    up, down = lax.rem(gx + nx - 1, nx), lax.rem(gx + 1, nx)
    left, right = lax.rem(gy + ny - 1, ny), lax.rem(gy + 1, ny)

    load_d = pltpu.make_async_copy(dens_hbm, dens.at[:, 0, WIDE : WIDE + ROWS], load_sem.at[0])
    load_c = pltpu.make_async_copy(cots_hbm, cots.at[:, 0, NEAR : NEAR + ROWS], load_sem.at[1])
    load_d.start()
    load_c.start()

    around = (
        (up, gy), (down, gy), (gx, left), (gx, right),
        (up, left), (up, right), (down, left), (down, right),
        (lax.rem(gx + 4, nx), gy), (lax.rem(gx + nx - 4, nx), gy), (gx + 3 - 2 * lax.rem(gx, 4), gy),
    )
    mine = rank(gx, gy)
    low_end, high_end = lax.rem(gx, 4) == 0, lax.rem(gx, 4) == 3
    at_end = jnp.logical_or(low_end, high_end)
    ends = (low_end, high_end, None, None, low_end, low_end, high_end, high_end)
    later, ready, earlier, greets = [], [], [], []
    for d, (x, y) in enumerate(around):
        lag = rank(x, y) - mine
        slack = 20 if d < 4 else 0 if d < 8 else 30
        if d < 8 and ends[d] is not None:
            slack = slack + (30 - slack) * ends[d].astype(jnp.int32)
        slack = slack * jnp.minimum(lax.rem(gy + 1, 16), 1) * jnp.minimum(lax.rem(y + 1, 16), 1)
        later.append(lag > slack)
        ready.append(lag <= slack)
        mutual = jnp.logical_and(lag <= slack, lag >= -slack)
        earlier.append(lag < -slack)
        greets.append(jnp.logical_or(lag > slack, mutual))
    for d in range(8, 11):
        for flags in (later, ready, earlier, greets):
            flags[d] = jnp.logical_and(at_end, flags[d])
    barrier = pltpu.get_barrier_semaphore()
    for d, (x, y) in enumerate(around):
        pl.when(greets[d])(
            lambda x=x, y=y: pl.semaphore_signal(
                barrier, inc=1, device_id={"gx": x, "gy": y}, device_id_type=MESH
            )
        )
    pl.semaphore_wait(barrier, sum(v.astype(jnp.int32) for v in ready))
    for d, (x, y) in enumerate(around):
        pl.when(earlier[d])(
            lambda d=d, x=x, y=y: pl.semaphore_signal(
                token_sem.at[OPPOSITE[d]], inc=1, device_id={"gx": x, "gy": y}, device_id_type=MESH
            )
        )

    bufs = (
        (dens, WIDE, (row_out_d, col_out_d, cor_out_d), (row_in_d, col_in_d, cor_in_d)),
        (cots, NEAR, (row_out_c, col_out_c, cor_out_c), (row_in_c, col_in_c, cor_in_c)),
    )

    def pack(which):
        plan = PLANS[which]
        src, margin, (row, col, cor), _ = bufs[which]
        for z in plan.order:
            w, at = plan.width(z), plan.starts[z]
            row[0, at : at + w, :] = src[z, 0, margin : margin + w, :]
            row[1, at : at + w, :] = src[z, 0, margin + ROWS - w : margin + ROWS, :]
        for vec in range(plan.col_vecs):
            lane = lane_ids((ROWS, LANES))
            low = high = None
            for z in plan.order:
                v, off = plan.cols[z]
                if v != vec:
                    continue
                w = plan.width(z)
                own = src[z, 0, margin : margin + ROWS, :]
                if low is None:
                    low, high = rotate(own, off), rotate(own, off + w)
                else:
                    low = jnp.where(lane >= off, rotate(own, off), low)
                    high = jnp.where(lane >= off, rotate(own, off + w), high)
            col[0, vec * ROWS : (vec + 1) * ROWS, :] = low
            col[1, vec * ROWS : (vec + 1) * ROWS, :] = high
        lane = lane_ids((8, LANES))
        for vec in range(plan.corner_vecs):
            for side in range(2):
                low = high = None
                for (z, b), (v, off, n) in plan.corners.items():
                    if v != vec:
                        continue
                    lo = margin + 8 * b if side == 0 else margin + ROWS - 8 * (b + 1)
                    own = src[z, 0, lo : lo + 8, :]
                    turned = rotate(own, off)
                    other = rotate(own, off + n) if plan.tight else turned
                    start, end = (off, LANES) if plan.tight else (off - n, off)
                    if low is None:
                        low, high = turned, other
                    else:
                        low = jnp.where(lane >= off, turned, low)
                        high = jnp.where((lane >= start) & (lane < end), other, high)
                cor[2 * side, 8 * vec : 8 * vec + 8, :] = low
                cor[2 * side + 1, 8 * vec : 8 * vec + 8, :] = high

    copies, order = ({}, {}), ([], [])
    relays, hops, vias = (relay_d, relay_c), [[] for _ in RELAYED], {}
    count = 0
    for which, plan in enumerate(PLANS):
        _, _, outs, ins = bufs[which]
        for kind, c in COPIES[which]:
            made = []
            if kind == "row":
                at, n = plan.row_chunks[c]
                targets = [(0, 0), (1, 1)]
                src, dst = outs[0], ins[0]
            elif kind == "col":
                at, n = c * ROWS, ROWS
                targets = [(0, 2), (1, 3)]
                src, dst = outs[1], ins[1]
            else:
                at, n = plan.corner_chunks[c]
                targets = [(0, 4), (1, 5), (2, 6), (3, 7)]
                src, dst = outs[2], ins[2]
            for i, d in targets:
                x, y = around[d]
                copy = (
                    pltpu.make_async_remote_copy(
                        src_ref=src.at[i, at : at + n],
                        dst_ref=dst.at[i, at : at + n],
                        send_sem=send_sem.at[8 * which + d],
                        recv_sem=recv_sem.at[count],
                        device_id={"gx": x, "gy": y},
                        device_id_type=MESH,
                    )
                )
                made.append(copy)
                if (which, c) in RELAYED and kind == "row":
                    k = RELAYED.index((which, c))
                    end, beyond = ((low_end, 9), (high_end, 8))[i]
                    x, y = around[10]
                    via = pltpu.make_async_remote_copy(
                        src_ref=src.at[i, at : at + n],
                        dst_ref=relays[which].at[at : at + n],
                        send_sem=send_sem.at[8 * which + d],
                        recv_sem=relay_recv.at[k],
                        device_id={"gx": x, "gy": y},
                        device_id_type=MESH,
                    )
                    x, y = around[beyond]
                    onward = pltpu.make_async_remote_copy(
                        src_ref=relays[which].at[at : at + n],
                        dst_ref=dst.at[i, at : at + n],
                        send_sem=relay_send.at[which],
                        recv_sem=recv_sem.at[count],
                        device_id={"gx": x, "gy": y},
                        device_id_type=MESH,
                    )
                    order[which].append((d, copy, jnp.logical_not(end)))
                    order[which].append((10, via, end))
                    hops[k].append(onward)
                    vias[k] = via
                else:
                    order[which].append((d, copy, None))
                count += 1
            copies[which][(kind, c)] = made

    def sent(src, dst, sem):
        pltpu.make_async_remote_copy(
            src_ref=src,
            dst_ref=dst,
            send_sem=sem,
            recv_sem=recv_sem.at[0],
            device_id={"gx": up, "gy": gy},
            device_id_type=MESH,
        ).wait_send()

    load_d.wait()
    pack(0)

    def send(which, d, gate):
        for e, copy, on in order[which]:
            if d is not None and e != d:
                continue
            conds = [v for v in (gate[e] if gate else None, on) if v is not None]
            if not conds:
                copy.start()
            else:
                pl.when(conds[0] if len(conds) == 1 else jnp.logical_and(*conds))(copy.start)

    feeds = lax.rem(gy, 16) == 15
    usual = jnp.logical_not(feeds)
    first = [v if d in URGENT else jnp.logical_and(v, usual) for d, v in enumerate(ready)]
    after = [jnp.logical_and(v, feeds) for v in ready]
    send(0, None, first)
    load_c.wait()
    pack(1)

    def gone():
        for d in URGENT[:2]:
            sent(cor_out_d.at[d - 4], cor_in_d.at[d - 4], send_sem.at[d])

    pl.when(feeds)(gone)
    for d in range(11):
        if d not in URGENT:
            send(0, d, after)
    send(1, None, ready)

    def answer(d):
        pl.semaphore_wait(token_sem.at[d], 1)
        send(0, d, None)
        send(1, d, None)

    for d in TOKEN_ORDER[:-3]:
        pl.when(later[d])(lambda d=d: answer(d))

    def pass_on(k):
        vias[k].wait_recv()
        pl.when(high_end)(hops[k][0].start)
        pl.when(low_end)(hops[k][1].start)

    waits = jnp.logical_and(at_end, later[2])
    busy = jnp.logical_and(at_end, jnp.logical_not(later[2]))
    for k, (which, _) in enumerate(RELAYED):
        pl.when(at_end if which == 0 else waits)(lambda k=k: pass_on(k))
    for d in TOKEN_ORDER[-3:]:
        pl.when(later[d])(lambda d=d: answer(d))

    arrived = (set(), set())

    def receive(which, z):
        plan = PLANS[which]
        dst, margin, _, (row, col, cor) = bufs[which]
        wanted = [("row", c) for c in range(plan.row_need[z] + 1)]
        wanted += [("corner", c) for c in range(plan.corner_need(z) + 1)]
        wanted += [("col", c) for c in range(plan.cols[z][0] + 1)]
        for m in wanted:
            if m not in arrived[which]:
                arrived[which].add(m)
                for copy in copies[which][m]:
                    copy.wait_recv()
        w, at = plan.width(z), plan.starts[z]
        dst[z, 0, margin + ROWS : margin + ROWS + w, :] = row[0, at : at + w, :]
        dst[z, 0, margin - w : margin, :] = row[1, at : at + w, :]
        vec, off = plan.cols[z]
        lane = lane_ids((ROWS, LANES))
        part = slice(vec * ROWS, (vec + 1) * ROWS)
        low, high = rotate(col[0, part, :], LANES - off), rotate(col[1, part, :], 2 * LANES - off - w)
        dst[z, 1, margin : margin + ROWS, :] = jnp.where(lane < LANES // 2, low, high)
        lane = lane_ids((8, LANES))
        for b in range(4):
            if (z, b) not in plan.corners:
                continue
            vec, off, n = plan.corners[(z, b)]
            part = slice(8 * vec, 8 * vec + 8)
            def merge(i):
                low, high = cor[i, part, :], cor[i + 1, part, :]
                if plan.tight:
                    low, high = rotate(low, LANES - off), rotate(high, 2 * LANES - off - n)
                    return jnp.where(lane < LANES // 2, low, high)
                return rotate(jnp.where((lane >= off) & (lane < off + n), low, high), LANES - off)

            lo = margin + ROWS + 8 * b
            dst[z, 1, lo : lo + 8, :] = merge(0)
            lo = margin - 8 * (b + 1)
            dst[z, 1, lo : lo + 8, :] = merge(2)

    towers = (t_even, t_odd)
    inner = WIDE - NEAR
    for z in range(NZ):
        for k in PASS_ON.get(z, []):
            pl.when(busy)(lambda k=k: pass_on(k))
        receive(0, z)
        below, above = towers[(z + 1) % 2], towers[z % 2]
        for lo, hi in spans(WIDE, up8(REACH[z])):
            plane = dens[z, :, lo:hi, :]
            if z == 0:
                level = jnp.ones_like(plane)
            else:
                total = cross(below, lo + 8, hi + 8)
                logs = jnp.log(total)
                level = jnp.exp(logs * (1.0 / root_q))
            diff = plane - level
            square = diff * diff + smooth_eps
            inverse = lax.rsqrt(square)
            layer = 0.5 * (plane + level - square * inverse) + 0.5 * math.sqrt(smooth_eps)
            p2 = layer * layer
            p4 = p2 * p2
            p8 = p4 * p4
            p16 = p8 * p8
            p19 = p16 * (p2 * layer)
            if z < NZ - 1:
                above[:, lo + 8 : hi + 8, :] = p19 * layer
            near_lo, near_hi = max(lo, WIDE - up8(z)), min(hi, WIDE + ROWS + up8(z))
            if near_lo < near_hi:
                cut = lambda v: v[:, near_lo - lo : near_hi - lo, :]
                tilt = 0.5 * (cut(diff) * cut(inverse))
                coef[z, :, near_lo - inner : near_hi - inner, :] = (power_p / root_q) * cut(p19)
                if z > 0:
                    weight[z, :, near_lo - inner : near_hi - inner, :] = (0.5 + tilt) * jnp.exp(
                        cut(logs) * (1.0 / root_q - 1.0)
                    )
                if WIDE <= lo and hi <= WIDE + ROWS:
                    printed_ref[z, lo - WIDE : hi - WIDE, :] = layer[0]
                    shrink[z, lo - WIDE : hi - WIDE, :] = 0.5 - tilt[0]

    carried = (k_even, k_odd)
    for z in reversed(range(NZ)):
        if z > 0:
            receive(1, z)
        above, here = carried[(z + 1) % 2], carried[z % 2]
        for lo, hi in spans(NEAR, up8(z)):
            if z == 0:
                adjoint = cots[z, 0, lo:hi, :] + coef[z, 0, lo:hi, :] * cross(above, lo + 8, hi + 8)[0]
            elif z == NZ - 1:
                adjoint = cots[z, :, lo:hi, :]
            else:
                adjoint = cots[z, :, lo:hi, :] + coef[z, :, lo:hi, :] * cross(above, lo + 8, hi + 8)
            if z > 0:
                here[:, lo + 8 : hi + 8, :] = adjoint * weight[z, :, lo:hi, :]
            if NEAR <= lo and hi <= NEAR + ROWS:
                own = adjoint if z == 0 else adjoint[0]
                rows = slice(lo - NEAR, hi - NEAR)
                grad_ref[z, rows, :] = own * shrink[z, rows, :]

    for which in range(2):
        _, _, outs, ins = bufs[which]
        for d in range(8):
            part, i = (0, d) if d < 2 else (1, d - 2) if d < 4 else (2, d - 4)
            args = (outs[part].at[i], ins[part].at[i], send_sem.at[8 * which + d])
            if which == 0 and d in URGENT[:2]:
                pl.when(usual)(lambda args=args: sent(*args))
            else:
                sent(*args)
        part = [PLANS[which].row_chunks[c] for w, c in RELAYED if w == which]
        lo, hi = part[0][0], part[-1][0] + part[-1][1]
        relay = relays[which].at[lo:hi]
        pl.when(at_end)(lambda relay=relay, which=which: sent(relay, relay, relay_send.at[which]))


def shards(density, cotangent):
    def packed(plan):
        out = []
        for shape in ((2, plan.rows, LANES), (2, plan.col_vecs * ROWS, LANES), (4, 8 * plan.corner_vecs, LANES)):
            out += [pltpu.VMEM(shape, F32)] * 2
        return out

    wide, near = 2 * WIDE + ROWS, 2 * NEAR + ROWS
    shape = pltpu.VMEM(density.shape, F32)
    results = pl.pallas_call(
        kernel,
        out_shape=(shape, shape),
        in_specs=[pl.BlockSpec(memory_space=pl.ANY)] * 2,
        out_specs=(pl.BlockSpec(memory_space=pltpu.VMEM),) * 2,
        scratch_shapes=[
            pltpu.VMEM((NZ, 2, wide, LANES), F32),
            pltpu.VMEM((NZ, 2, near, LANES), F32),
            pltpu.VMEM((2, wide + 16, LANES), F32),
            pltpu.VMEM((2, wide + 16, LANES), F32),
            pltpu.VMEM((2, near + 16, LANES), F32),
            pltpu.VMEM((2, near + 16, LANES), F32),
            pltpu.VMEM((NZ, 2, near, LANES), F32),
            pltpu.VMEM((NZ, 2, near, LANES), F32),
            pltpu.VMEM((NZ, ROWS, LANES), F32),
            pltpu.VMEM((DENS.rows, LANES), F32),
            pltpu.VMEM((COTS.rows, LANES), F32),
            *packed(DENS),
            *packed(COTS),
            pltpu.SemaphoreType.DMA((2,)),
            pltpu.SemaphoreType.DMA((16,)),
            pltpu.SemaphoreType.DMA((N_SEMS,)),
            pltpu.SemaphoreType.REGULAR((11,)),
            pltpu.SemaphoreType.DMA((2,)),
            pltpu.SemaphoreType.DMA((len(RELAYED),)),
        ],
        compiler_params=pltpu.CompilerParams(collective_id=0, has_side_effects=True),
    )(density, cotangent)
    final = jax.ShapeDtypeStruct(density.shape, F32)
    return pl.pallas_call(
        store,
        out_shape=(final, final),
        in_specs=[pl.BlockSpec(memory_space=pltpu.VMEM)] * 2,
        out_specs=(pl.BlockSpec(memory_space=pl.ANY),) * 2,
        scratch_shapes=[pltpu.SemaphoreType.DMA((8,))],
    )(*(pltpu.with_memory_space_constraint(v, pltpu.VMEM) for v in results))


def store(printed_ref, grad_ref, printed_hbm, grad_hbm, sem):
    copies = []
    for i in range(8):
        src, dst = ((printed_ref, printed_hbm), (grad_ref, grad_hbm))[i % 2]
        part = slice(4 * (i // 2), 4 * (i // 2) + 4)
        copies.append(pltpu.make_async_copy(src.at[part], dst.at[part], sem.at[i]))
    for copy in copies:
        copy.start()
    for copy in copies:
        copy.wait()


def solution(mesh):
    placed = (P(None, "gx", "gy"), P(None, "gx", "gy"))
    return jax.shard_map(
        shards,
        mesh=mesh,
        in_specs=placed,
        out_specs=placed,
        check_vma=False,
    )
```

```python
import functools
import math

import jax
import jax.numpy as jnp
from jax import lax
from jax.experimental import pallas as pl
from jax.experimental.pallas import tpu as pltpu
from jax.sharding import PartitionSpec as P

power_p = 20.0
root_q = 20.0 + math.log(5.0) / math.log(0.1)
smooth_eps = 0.0001

NZ = 16
ROWS = 64
LANES = 128
WIDE = 32
NEAR = 16
F32 = jnp.float32
MESH = pl.DeviceIdType.MESH

REACH = [2 * (NZ - 1) - z for z in range(NZ)]


def up8(n):
    return (n + 7) // 8 * 8


def place(counts, tight):
    out, vec, first, last, prev = [], 0, None, 0, 0
    for n in counts:
        if first is None:
            off, first = 0, n
        else:
            off = last + (prev if tight else max(prev, n))
            if off + n > LANES or (off > LANES - first and not tight):
                vec, off, first = vec + 1, 0, n
        out.append((vec, off))
        last, prev = off, n
    return out, vec + 1


def stream(order, width):
    starts, chunks, at, sent = {}, [], 0, 0
    for z in order:
        starts[z] = at
        at += width(z)
        end = up8(at)
        chunks.append((sent, end - sent))
        sent = end
    return starts, chunks, sent


class Plan:
    def __init__(self, order, width, merges, groups, tight):
        self.order, self.width = order, width
        self.starts, chunks, self.rows = stream(order, width)
        self.row_chunks, self.row_need, at = [], {}, 0
        for count in merges:
            part = chunks[at : at + count]
            for z in order[at : at + count]:
                self.row_need[z] = len(self.row_chunks)
            self.row_chunks.append((part[0][0], sum(n for _, n in part)))
            at += count
        places, self.col_vecs = place([width(z) for z in order], True)
        self.cols = {z: p for z, p in zip(order, places)}
        self.corners, base = {}, 0
        firsts = []
        self.tight = tight
        for bands in groups:
            items = [
                (z, b, width(z) - 8 * b - 1)
                for b in bands
                for z in order
                if width(z) - 8 * b - 1 > 0
            ]
            if not items:
                continue
            places, vecs = place([n for _, _, n in items], tight)
            for (z, b, n), (vec, off) in zip(items, places):
                self.corners[(z, b)] = (base + vec, off, n)
            for vec in range(vecs):
                firsts.append(min(order.index(z) for (z, b, n), p in zip(items, places) if p[0] == vec))
            base += vecs
        rank = sorted(range(base), key=lambda v: firsts[v])
        where = {v: i for i, v in enumerate(rank)}
        self.corners = {k: (where[v], o, n) for k, (v, o, n) in self.corners.items()}
        self.corner_vecs = base
        self.corner_chunks, self.corner_first = [], []
        for i, v in enumerate(rank):
            if self.corner_first and firsts[v] == self.corner_first[-1]:
                at, n = self.corner_chunks[-1]
                self.corner_chunks[-1] = (at, n + 8)
            else:
                self.corner_chunks.append((8 * i, 8))
                self.corner_first.append(firsts[v])

    def corner_need(self, z):
        need = -1
        for (layer, _), (vec, _, _) in self.corners.items():
            if layer == z:
                for i, (at, n) in enumerate(self.corner_chunks):
                    if at <= 8 * vec < at + n:
                        need = max(need, i)
        return need


DENS = Plan(list(range(NZ)), lambda z: REACH[z], [1] * 8 + [2] * 4, ((0,), (1,), (2, 3)), False)
COTS = Plan(list(range(NZ - 1, 0, -1)), lambda z: z, [1, 1, 2, 4, 7], ((0, 1),), True)
PLANS = (DENS, COTS)

RELAYED = [(0, 8), (0, 9), (0, 10), (0, 11), (1, 0), (1, 1), (1, 2), (1, 3), (1, 4)]
PASS_ON = {1: [4], 2: [5], 3: [6], 4: [7], 5: [8]}


def messages(plan):
    out, seen = [], set()
    for i, z in enumerate(plan.order):
        wanted = [("corner", c) for c in range(len(plan.corner_chunks))]
        wanted += [("row", plan.row_need[z])]
        wanted += [("col", plan.cols[z][0])]
        for m in wanted:
            if m not in seen:
                seen.add(m)
                out.append(m)
    return out


COPIES = [messages(plan) for plan in PLANS]
SLOTS = [[(kind, c) for kind, c in copies for _ in range(4 if kind == "corner" else 2)] for copies in COPIES]
N_SEMS = sum(len(s) for s in SLOTS)


OPPOSITE = (1, 0, 3, 2, 7, 6, 5, 4, 9, 8, 10)
URGENT = (7, 5, 3)
TOKEN_ORDER = (3, 1, 10, 7, 0, 8, 9, 5, 2, 6, 4)


def rank(gx, gy):
    x, y = lax.rem(gx, 4), 2 * lax.div(gx, 4) + lax.div(gy, 16)
    z, core = lax.rem(lax.div(gy, 2), 8), lax.rem(gy, 2)
    far, deep = lax.div(y, 4), lax.div(z, 4)
    along_y = 6 * y * (1 - far) + (15 + 3 * (8 - y)) * far
    along_z = 13 * z * (1 - deep) + (41 + 5 * z) * deep
    first = 1 - lax.div(gx * 32 + gy + 511, 512)
    return along_z + along_y + 4 * x + 6 * (1 - core) + 60 * first


def lane_ids(shape):
    return lax.broadcasted_iota(jnp.int32, shape, len(shape) - 1)


def rotate(x, shift, axis=None):
    shift = shift % LANES
    if shift == 0:
        return x
    return pltpu.roll(x, shift, x.ndim - 1 if axis is None else axis)


def cross(ref, lo, hi):
    here = ref[:, lo:hi, :]
    lane = lane_ids(here.shape)
    east = rotate(here, 1)
    west = rotate(here, LANES - 1)
    swap = lambda v: jnp.concatenate([v[1:], v[:1]], axis=0)
    return (
        here
        + ref[:, lo - 1 : hi - 1, :]
        + ref[:, lo + 1 : hi + 1, :]
        + jnp.where(lane == 0, swap(east), east)
        + jnp.where(lane == LANES - 1, swap(west), west)
    )


def spans(margin, halo):
    out = []
    if halo:
        out.append((margin - halo, margin))
    out += [(margin, margin + ROWS // 2), (margin + ROWS // 2, margin + ROWS)]
    if halo:
        out.append((margin + ROWS, margin + ROWS + halo))
    return out


def kernel(
    dens_hbm,
    cots_hbm,
    printed_ref,
    grad_ref,
    dens,
    cots,
    t_even,
    t_odd,
    k_even,
    k_odd,
    coef,
    weight,
    shrink,
    relay_d,
    relay_c,
    row_out_d,
    row_in_d,
    col_out_d,
    col_in_d,
    cor_out_d,
    cor_in_d,
    row_out_c,
    row_in_c,
    col_out_c,
    col_in_c,
    cor_out_c,
    cor_in_c,
    load_sem,
    send_sem,
    recv_sem,
    token_sem,
    relay_send,
    relay_recv,
):
    gx, gy = lax.axis_index("gx"), lax.axis_index("gy")
    nx, ny = lax.axis_size("gx"), lax.axis_size("gy")
    up, down = lax.rem(gx + nx - 1, nx), lax.rem(gx + 1, nx)
    left, right = lax.rem(gy + ny - 1, ny), lax.rem(gy + 1, ny)

    load_d = pltpu.make_async_copy(dens_hbm, dens.at[:, 0, WIDE : WIDE + ROWS], load_sem.at[0])
    load_c = pltpu.make_async_copy(cots_hbm, cots.at[:, 0, NEAR : NEAR + ROWS], load_sem.at[1])
    load_d.start()
    load_c.start()

    around = (
        (up, gy), (down, gy), (gx, left), (gx, right),
        (up, left), (up, right), (down, left), (down, right),
        (lax.rem(gx + 4, nx), gy), (lax.rem(gx + nx - 4, nx), gy), (gx + 3 - 2 * lax.rem(gx, 4), gy),
    )
    mine = rank(gx, gy)
    low_end, high_end = lax.rem(gx, 4) == 0, lax.rem(gx, 4) == 3
    at_end = jnp.logical_or(low_end, high_end)
    ends = (low_end, high_end, None, None, low_end, low_end, high_end, high_end)
    later, ready, earlier, greets = [], [], [], []
    for d, (x, y) in enumerate(around):
        lag = rank(x, y) - mine
        slack = 20 if d < 4 else 0 if d < 8 else 30
        if d < 8 and ends[d] is not None:
            slack = slack + (30 - slack) * ends[d].astype(jnp.int32)
        slack = slack * jnp.minimum(lax.rem(gy + 1, 16), 1) * jnp.minimum(lax.rem(y + 1, 16), 1)
        later.append(lag > slack)
        ready.append(lag <= slack)
        mutual = jnp.logical_and(lag <= slack, lag >= -slack)
        earlier.append(lag < -slack)
        greets.append(jnp.logical_or(lag > slack, mutual))
    for d in range(8, 11):
        for flags in (later, ready, earlier, greets):
            flags[d] = jnp.logical_and(at_end, flags[d])
    barrier = pltpu.get_barrier_semaphore()
    for d, (x, y) in enumerate(around):
        pl.when(greets[d])(
            lambda x=x, y=y: pl.semaphore_signal(
                barrier, inc=1, device_id={"gx": x, "gy": y}, device_id_type=MESH
            )
        )
    pl.semaphore_wait(barrier, sum(v.astype(jnp.int32) for v in ready))
    for d, (x, y) in enumerate(around):
        pl.when(earlier[d])(
            lambda d=d, x=x, y=y: pl.semaphore_signal(
                token_sem.at[OPPOSITE[d]], inc=1, device_id={"gx": x, "gy": y}, device_id_type=MESH
            )
        )

    bufs = (
        (dens, WIDE, (row_out_d, col_out_d, cor_out_d), (row_in_d, col_in_d, cor_in_d)),
        (cots, NEAR, (row_out_c, col_out_c, cor_out_c), (row_in_c, col_in_c, cor_in_c)),
    )

    def pack(which):
        plan = PLANS[which]
        src, margin, (row, col, cor), _ = bufs[which]
        for z in plan.order:
            w, at = plan.width(z), plan.starts[z]
            row[0, at : at + w, :] = src[z, 0, margin : margin + w, :]
            row[1, at : at + w, :] = src[z, 0, margin + ROWS - w : margin + ROWS, :]
        for vec in range(plan.col_vecs):
            lane = lane_ids((ROWS, LANES))
            low = high = None
            for z in plan.order:
                v, off = plan.cols[z]
                if v != vec:
                    continue
                w = plan.width(z)
                own = src[z, 0, margin : margin + ROWS, :]
                if low is None:
                    low, high = rotate(own, off), rotate(own, off + w)
                else:
                    low = jnp.where(lane >= off, rotate(own, off), low)
                    high = jnp.where(lane >= off, rotate(own, off + w), high)
            col[0, vec * ROWS : (vec + 1) * ROWS, :] = low
            col[1, vec * ROWS : (vec + 1) * ROWS, :] = high
        lane = lane_ids((8, LANES))
        for vec in range(plan.corner_vecs):
            for side in range(2):
                low = high = None
                for (z, b), (v, off, n) in plan.corners.items():
                    if v != vec:
                        continue
                    lo = margin + 8 * b if side == 0 else margin + ROWS - 8 * (b + 1)
                    own = src[z, 0, lo : lo + 8, :]
                    turned = rotate(own, off)
                    other = rotate(own, off + n) if plan.tight else turned
                    start, end = (off, LANES) if plan.tight else (off - n, off)
                    if low is None:
                        low, high = turned, other
                    else:
                        low = jnp.where(lane >= off, turned, low)
                        high = jnp.where((lane >= start) & (lane < end), other, high)
                cor[2 * side, 8 * vec : 8 * vec + 8, :] = low
                cor[2 * side + 1, 8 * vec : 8 * vec + 8, :] = high

    copies, order = ({}, {}), ([], [])
    relays, hops, vias = (relay_d, relay_c), [[] for _ in RELAYED], {}
    count = 0
    for which, plan in enumerate(PLANS):
        _, _, outs, ins = bufs[which]
        for kind, c in COPIES[which]:
            made = []
            if kind == "row":
                at, n = plan.row_chunks[c]
                targets = [(0, 0), (1, 1)]
                src, dst = outs[0], ins[0]
            elif kind == "col":
                at, n = c * ROWS, ROWS
                targets = [(0, 2), (1, 3)]
                src, dst = outs[1], ins[1]
            else:
                at, n = plan.corner_chunks[c]
                targets = [(0, 4), (1, 5), (2, 6), (3, 7)]
                src, dst = outs[2], ins[2]
            for i, d in targets:
                x, y = around[d]
                copy = (
                    pltpu.make_async_remote_copy(
                        src_ref=src.at[i, at : at + n],
                        dst_ref=dst.at[i, at : at + n],
                        send_sem=send_sem.at[8 * which + d],
                        recv_sem=recv_sem.at[count],
                        device_id={"gx": x, "gy": y},
                        device_id_type=MESH,
                    )
                )
                made.append(copy)
                if (which, c) in RELAYED and kind == "row":
                    k = RELAYED.index((which, c))
                    end, beyond = ((low_end, 9), (high_end, 8))[i]
                    x, y = around[10]
                    via = pltpu.make_async_remote_copy(
                        src_ref=src.at[i, at : at + n],
                        dst_ref=relays[which].at[at : at + n],
                        send_sem=send_sem.at[8 * which + d],
                        recv_sem=relay_recv.at[k],
                        device_id={"gx": x, "gy": y},
                        device_id_type=MESH,
                    )
                    x, y = around[beyond]
                    onward = pltpu.make_async_remote_copy(
                        src_ref=relays[which].at[at : at + n],
                        dst_ref=dst.at[i, at : at + n],
                        send_sem=relay_send.at[which],
                        recv_sem=recv_sem.at[count],
                        device_id={"gx": x, "gy": y},
                        device_id_type=MESH,
                    )
                    order[which].append((d, copy, jnp.logical_not(end)))
                    order[which].append((10, via, end))
                    hops[k].append(onward)
                    vias[k] = via
                else:
                    order[which].append((d, copy, None))
                count += 1
            copies[which][(kind, c)] = made

    def sent(src, dst, sem):
        pltpu.make_async_remote_copy(
            src_ref=src,
            dst_ref=dst,
            send_sem=sem,
            recv_sem=recv_sem.at[0],
            device_id={"gx": up, "gy": gy},
            device_id_type=MESH,
        ).wait_send()

    load_d.wait()
    pack(0)

    def send(which, d, gate):
        for e, copy, on in order[which]:
            if d is not None and e != d:
                continue
            conds = [v for v in (gate[e] if gate else None, on) if v is not None]
            if not conds:
                copy.start()
            else:
                pl.when(conds[0] if len(conds) == 1 else jnp.logical_and(*conds))(copy.start)

    feeds = lax.rem(gy, 16) == 15
    usual = jnp.logical_not(feeds)
    holds = jnp.logical_and(at_end, lax.rem(lax.div(gy, 2), 8) == 7)
    freed = jnp.logical_not(holds)
    held = {}
    for d, end in enumerate(ends):
        if end is not None:
            held[d] = jnp.logical_and(end, holds)
            if d in URGENT:
                held[d] = jnp.logical_and(held[d], usual)

    def gated(gate, *more):
        return functools.reduce(jnp.logical_and, more, gate)

    first, after, last = [], [], []
    for d, v in enumerate(ready):
        loose = (jnp.logical_not(held[d]),) if d in held else ()
        first.append(gated(v, *loose) if d in URGENT else gated(v, usual, *loose))
        after.append(gated(v, feeds, *loose))
        last.append(gated(v, held[d]) if d in held else None)
    send(0, None, first)
    load_c.wait()
    pack(1)

    def gone():
        for d in URGENT[:2]:
            sent(cor_out_d.at[d - 4], cor_in_d.at[d - 4], send_sem.at[d])

    pl.when(feeds)(gone)
    for d in range(11):
        if d not in URGENT:
            send(0, d, after)

    def columns():
        for c in range(DENS.col_vecs):
            copies[0][("col", c)][1].wait_recv()

    pl.when(holds)(columns)
    for d in held:
        send(0, d, last)
    send(1, None, ready)

    def answer(d):
        pl.semaphore_wait(token_sem.at[d], 1)
        send(0, d, None)
        send(1, d, None)

    for d in TOKEN_ORDER[:-3]:
        pl.when(later[d])(lambda d=d: answer(d))

    def pass_on(k):
        vias[k].wait_recv()
        pl.when(high_end)(hops[k][0].start)
        pl.when(low_end)(hops[k][1].start)

    waits = jnp.logical_and(at_end, later[2])
    busy = jnp.logical_and(at_end, jnp.logical_not(later[2]))
    for k, (which, _) in enumerate(RELAYED):
        pl.when(at_end if which == 0 else waits)(lambda k=k: pass_on(k))
    for d in TOKEN_ORDER[-3:]:
        pl.when(later[d])(lambda d=d: answer(d))

    arrived = (set(), set())

    def receive(which, z):
        plan = PLANS[which]
        dst, margin, _, (row, col, cor) = bufs[which]
        wanted = [("row", c) for c in range(plan.row_need[z] + 1)]
        wanted += [("corner", c) for c in range(plan.corner_need(z) + 1)]
        wanted += [("col", c) for c in range(plan.cols[z][0] + 1)]
        for m in wanted:
            if m not in arrived[which]:
                arrived[which].add(m)
                for i, copy in enumerate(copies[which][m]):
                    if which == 0 and m[0] == "col" and i == 1:
                        pl.when(freed)(copy.wait_recv)
                    else:
                        copy.wait_recv()
        w, at = plan.width(z), plan.starts[z]
        dst[z, 0, margin + ROWS : margin + ROWS + w, :] = row[0, at : at + w, :]
        dst[z, 0, margin - w : margin, :] = row[1, at : at + w, :]
        vec, off = plan.cols[z]
        lane = lane_ids((ROWS, LANES))
        part = slice(vec * ROWS, (vec + 1) * ROWS)
        low, high = rotate(col[0, part, :], LANES - off), rotate(col[1, part, :], 2 * LANES - off - w)
        dst[z, 1, margin : margin + ROWS, :] = jnp.where(lane < LANES // 2, low, high)
        lane = lane_ids((8, LANES))
        for b in range(4):
            if (z, b) not in plan.corners:
                continue
            vec, off, n = plan.corners[(z, b)]
            part = slice(8 * vec, 8 * vec + 8)
            def merge(i):
                low, high = cor[i, part, :], cor[i + 1, part, :]
                if plan.tight:
                    low, high = rotate(low, LANES - off), rotate(high, 2 * LANES - off - n)
                    return jnp.where(lane < LANES // 2, low, high)
                return rotate(jnp.where((lane >= off) & (lane < off + n), low, high), LANES - off)

            lo = margin + ROWS + 8 * b
            dst[z, 1, lo : lo + 8, :] = merge(0)
            lo = margin - 8 * (b + 1)
            dst[z, 1, lo : lo + 8, :] = merge(2)

    towers = (t_even, t_odd)
    inner = WIDE - NEAR
    for z in range(NZ):
        for k in PASS_ON.get(z, []):
            pl.when(busy)(lambda k=k: pass_on(k))
        receive(0, z)
        below, above = towers[(z + 1) % 2], towers[z % 2]
        for lo, hi in spans(WIDE, up8(REACH[z])):
            plane = dens[z, :, lo:hi, :]
            if z == 0:
                level = jnp.ones_like(plane)
            else:
                total = cross(below, lo + 8, hi + 8)
                logs = jnp.log(total)
                level = jnp.exp(logs * (1.0 / root_q))
            diff = plane - level
            square = diff * diff + smooth_eps
            inverse = lax.rsqrt(square)
            layer = 0.5 * (plane + level - square * inverse) + 0.5 * math.sqrt(smooth_eps)
            p2 = layer * layer
            p4 = p2 * p2
            p8 = p4 * p4
            p16 = p8 * p8
            p19 = p16 * (p2 * layer)
            if z < NZ - 1:
                above[:, lo + 8 : hi + 8, :] = p19 * layer
            near_lo, near_hi = max(lo, WIDE - up8(z)), min(hi, WIDE + ROWS + up8(z))
            if near_lo < near_hi:
                cut = lambda v: v[:, near_lo - lo : near_hi - lo, :]
                tilt = 0.5 * (cut(diff) * cut(inverse))
                coef[z, :, near_lo - inner : near_hi - inner, :] = (power_p / root_q) * cut(p19)
                if z > 0:
                    weight[z, :, near_lo - inner : near_hi - inner, :] = (0.5 + tilt) * jnp.exp(
                        cut(logs) * (1.0 / root_q - 1.0)
                    )
                if WIDE <= lo and hi <= WIDE + ROWS:
                    printed_ref[z, lo - WIDE : hi - WIDE, :] = layer[0]
                    shrink[z, lo - WIDE : hi - WIDE, :] = 0.5 - tilt[0]

    carried = (k_even, k_odd)
    for z in reversed(range(NZ)):
        if z > 0:
            receive(1, z)
        above, here = carried[(z + 1) % 2], carried[z % 2]
        for lo, hi in spans(NEAR, up8(z)):
            if z == 0:
                adjoint = cots[z, 0, lo:hi, :] + coef[z, 0, lo:hi, :] * cross(above, lo + 8, hi + 8)[0]
            elif z == NZ - 1:
                adjoint = cots[z, :, lo:hi, :]
            else:
                adjoint = cots[z, :, lo:hi, :] + coef[z, :, lo:hi, :] * cross(above, lo + 8, hi + 8)
            if z > 0:
                here[:, lo + 8 : hi + 8, :] = adjoint * weight[z, :, lo:hi, :]
            if NEAR <= lo and hi <= NEAR + ROWS:
                own = adjoint if z == 0 else adjoint[0]
                rows = slice(lo - NEAR, hi - NEAR)
                grad_ref[z, rows, :] = own * shrink[z, rows, :]

    for which in range(2):
        _, _, outs, ins = bufs[which]
        for d in range(8):
            part, i = (0, d) if d < 2 else (1, d - 2) if d < 4 else (2, d - 4)
            args = (outs[part].at[i], ins[part].at[i], send_sem.at[8 * which + d])
            if which == 0 and d in URGENT[:2]:
                pl.when(usual)(lambda args=args: sent(*args))
            else:
                sent(*args)
        part = [PLANS[which].row_chunks[c] for w, c in RELAYED if w == which]
        lo, hi = part[0][0], part[-1][0] + part[-1][1]
        relay = relays[which].at[lo:hi]
        pl.when(at_end)(lambda relay=relay, which=which: sent(relay, relay, relay_send.at[which]))


def shards(density, cotangent):
    def packed(plan):
        out = []
        for shape in ((2, plan.rows, LANES), (2, plan.col_vecs * ROWS, LANES), (4, 8 * plan.corner_vecs, LANES)):
            out += [pltpu.VMEM(shape, F32)] * 2
        return out

    wide, near = 2 * WIDE + ROWS, 2 * NEAR + ROWS
    shape = pltpu.VMEM(density.shape, F32)
    results = pl.pallas_call(
        kernel,
        out_shape=(shape, shape),
        in_specs=[pl.BlockSpec(memory_space=pl.ANY)] * 2,
        out_specs=(pl.BlockSpec(memory_space=pltpu.VMEM),) * 2,
        scratch_shapes=[
            pltpu.VMEM((NZ, 2, wide, LANES), F32),
            pltpu.VMEM((NZ, 2, near, LANES), F32),
            pltpu.VMEM((2, wide + 16, LANES), F32),
            pltpu.VMEM((2, wide + 16, LANES), F32),
            pltpu.VMEM((2, near + 16, LANES), F32),
            pltpu.VMEM((2, near + 16, LANES), F32),
            pltpu.VMEM((NZ, 2, near, LANES), F32),
            pltpu.VMEM((NZ, 2, near, LANES), F32),
            pltpu.VMEM((NZ, ROWS, LANES), F32),
            pltpu.VMEM((DENS.rows, LANES), F32),
            pltpu.VMEM((COTS.rows, LANES), F32),
            *packed(DENS),
            *packed(COTS),
            pltpu.SemaphoreType.DMA((2,)),
            pltpu.SemaphoreType.DMA((16,)),
            pltpu.SemaphoreType.DMA((N_SEMS,)),
            pltpu.SemaphoreType.REGULAR((11,)),
            pltpu.SemaphoreType.DMA((2,)),
            pltpu.SemaphoreType.DMA((len(RELAYED),)),
        ],
        compiler_params=pltpu.CompilerParams(collective_id=0, has_side_effects=True),
    )(density, cotangent)
    final = jax.ShapeDtypeStruct(density.shape, F32)
    return pl.pallas_call(
        store,
        out_shape=(final, final),
        in_specs=[pl.BlockSpec(memory_space=pltpu.VMEM)] * 2,
        out_specs=(pl.BlockSpec(memory_space=pl.ANY),) * 2,
        scratch_shapes=[pltpu.SemaphoreType.DMA((8,))],
    )(*(pltpu.with_memory_space_constraint(v, pltpu.VMEM) for v in results))


def store(printed_ref, grad_ref, printed_hbm, grad_hbm, sem):
    copies = []
    for i in range(8):
        src, dst = ((printed_ref, printed_hbm), (grad_ref, grad_hbm))[i % 2]
        part = slice(4 * (i // 2), 4 * (i // 2) + 4)
        copies.append(pltpu.make_async_copy(src.at[part], dst.at[part], sem.at[i]))
    for copy in copies:
        copy.start()
    for copy in copies:
        copy.wait()


def solution(mesh):
    placed = (P(None, "gx", "gy"), P(None, "gx", "gy"))
    return jax.shard_map(
        shards,
        mesh=mesh,
        in_specs=placed,
        out_specs=placed,
        check_vma=False,
    )
```
